32 devices in a mesh: pipe: 4 (over z), dp: 2 (over core), expert: 4 (over y, x).
Axes of the slice: x: 2, y: 2, z: 4, core: 2. Of those that a mesh axis runs over, the one named last changes fastest.
Arguments:
- cotangent: bfloat16 [4, 512, 7168], P('pipe', ('dp', 'expert')), may hold values from -6 to 6
- routes: int32 [4, 2, 512, 8], P('pipe', None, ('dp', 'expert')), may hold values from 0 to 255, as said below
- gates: bfloat16 [4, 2, 512, 8], P('pipe', None, ('dp', 'expert')), may hold values from 0.099609375 to 1
- gate_pre: bfloat16 [4, 2, 2, 4, 2, 4096], P('pipe', None, 'dp', None, None, 'expert'), may hold values from -6 to 6
- up_pre: bfloat16 [4, 2, 2, 4, 2, 4096], P('pipe', None, 'dp', None, None, 'expert'), may hold values from -6 to 6
- w_gate: bfloat16 [4, 7168, 4096], P('pipe', None, 'expert'), may hold values from -0.0625 to 0.0625
- w_up: bfloat16 [4, 7168, 4096], P('pipe', None, 'expert'), may hold values from -0.0625 to 0.0625
- w_down: bfloat16 [4, 4096, 7168], P('pipe', 'expert'), may hold values from -0.125 to 0.125
Outputs:
- down_grad: float32 [4, 4096, 7168], P('pipe', 'expert', 'dp')
The draws below stay inside these ranges and needn't reach their ends.
Inputs may be any that keep to these rules, and one draw needn't show every extreme that they name: `routes`: each token names 8 different experts. At one section and step the tokens of one device name each of the experts 0 to 1 at least once and at most 2 times; at every section and step, in some replica every device names one of them exactly 2 times.
All inputs are finite; a program needn't handle non-finite values.
Results may differ from the reference program's by a relative error of at most 0.0095.
Values may be sent and summed in bfloat16 or wider, within the bound.
A program may use at most 128 MiB of HBM per device.

```python
import math
import jax
import jax.numpy as jnp
from jax import lax

D = 7168
FFE = 2048
EXPERTS = 256
TOPK = 8
EXP_FL = 2
STEPS = 2
TOK_DEV = 64
CAP = 2
TOKENS = 512
N_PIPE = 4
N_DP = 2
N_EXPERT = 4


def draw_routes(key, part):
    keys = jax.random.split(key, 6)
    lead = (N_PIPE, STEPS, N_DP, N_EXPERT)
    counts = jax.random.randint(keys[0], lead + (EXP_FL,), 1, CAP + 1)
    full_rep = jax.random.randint(keys[1], (N_PIPE, STEPS, 1, 1, 1), 0, N_DP)
    full_exp = jax.random.randint(keys[2], (N_PIPE, STEPS, 1, 1, 1), 0, EXP_FL)
    rep_index = jnp.arange(N_DP).reshape(1, 1, N_DP, 1, 1)
    exp_index = jnp.arange(EXP_FL).reshape(1, 1, 1, 1, EXP_FL)
    counts = jnp.where((rep_index == full_rep) & (exp_index == full_exp), CAP, counts)
    scores = jax.random.randint(keys[3], lead + (EXP_FL, TOK_DEV), 0, 1 << 20) * TOK_DEV + jnp.arange(TOK_DEV)
    ranking = jnp.argsort(jnp.argsort(scores, axis=-1), axis=-1)
    chosen = ranking < counts[..., None]
    chosen = jnp.moveaxis(chosen, -2, -1)
    others = jax.random.randint(keys[4], lead + (TOK_DEV, EXPERTS - EXP_FL), 0, 1 << 16) * EXPERTS + jnp.arange(EXPERTS - EXP_FL)
    picked = lax.top_k(others, TOPK)[1] + EXP_FL
    head = jnp.where(chosen, jnp.arange(EXP_FL), picked[..., :EXP_FL])
    named = jnp.concatenate([head, picked[..., EXP_FL:]], axis=-1)
    order = jax.random.randint(keys[5], lead + (TOK_DEV, TOPK), 0, 1 << 20) * TOPK + jnp.arange(TOPK)
    shuffle = jnp.argsort(order, axis=-1)
    named = jnp.take_along_axis(named, shuffle, axis=-1)
    return named.reshape(N_PIPE, STEPS, N_DP * N_EXPERT * TOK_DEV, TOPK).astype(jnp.int32)


def steps_of(own_key, shape, cuts, least, largest):
    def one(axis_at, shards_of):
        heights = jax.random.uniform(jax.random.fold_in(jax.random.fold_in(own_key, 6), axis_at), (shards_of,), jnp.float32, least / len(cuts), largest / len(cuts))
        return jnp.repeat(jnp.exp(heights), shape[axis_at] // shards_of).reshape((-1,) + (1,) * (len(shape) - axis_at - 1))

    level = one(*cuts[0])
    for cut in cuts[1:]:
        level = level * one(*cut)
    return level


def scatter_about(rng, dims, scale, reach, pieces=(), held_as=jnp.bfloat16):
    entries = scale * jax.random.normal(rng, dims, jnp.float32)
    if pieces:
        entries = entries * steps_of(rng, dims, pieces, -0.22, 0.18)
    return jnp.clip(entries, -reach, reach).astype(held_as)


def setup_inputs(seed: int = 0) -> dict:
    arg_keys = jax.random.split(jax.random.key(seed), 9)
    cotangent = scatter_about(arg_keys[0], (N_PIPE, TOKENS, D), 1.0, 6.0, ((0, 4), (1, 8)))
    routes = draw_routes(jax.random.fold_in(arg_keys[8], 71), 0)
    gates = jnp.clip(jnp.exp(math.log(1.0) - 2.306499 * jax.random.uniform(arg_keys[2], (N_PIPE, STEPS, TOKENS, TOPK), jnp.float32) ** steps_of(arg_keys[2], (N_PIPE, STEPS, TOKENS, TOPK), ((0, 4), (2, 8)), -0.2, 0.2)), 0.099609375, 1.0).astype(jnp.bfloat16)
    gate_pre = scatter_about(arg_keys[3], (N_PIPE, STEPS, N_DP, N_EXPERT, CAP, EXP_FL * FFE), 1.0, 6.0, ((0, 4), (2, 2), (5, 4)))
    up_pre = scatter_about(arg_keys[4], (N_PIPE, STEPS, N_DP, N_EXPERT, CAP, EXP_FL * FFE), 1.0, 6.0, ((0, 4), (2, 2), (5, 4)))
    w_gate = scatter_about(arg_keys[5], (N_PIPE, D, EXP_FL * FFE), D ** -0.5, 0.0625, ((0, 4), (2, 4)))
    w_up = scatter_about(arg_keys[6], (N_PIPE, D, EXP_FL * FFE), D ** -0.5, 0.0625, ((0, 4), (2, 4)))
    w_down = scatter_about(arg_keys[7], (N_PIPE, EXP_FL * FFE, D), FFE ** -0.5, 0.125, ((0, 4), (1, 4)))
    return {"cotangent": cotangent, "routes": routes, "gates": gates, "gate_pre": gate_pre, "up_pre": up_pre, "w_gate": w_gate, "w_up": w_up, "w_down": w_down}


def slot_tables(ids, weights):
    match = (ids[..., None] == jnp.arange(EXP_FL, dtype=jnp.int32)).astype(jnp.float32)
    hit = jnp.sum(match, axis=2)
    gate_sum = jnp.sum(match * weights.astype(jnp.float32)[..., None, None].reshape(match.shape[:3] + (1,)), axis=2)
    rank = jnp.cumsum(hit, axis=1) - 1.0
    slots = jnp.arange(CAP, dtype=jnp.float32)
    select = hit[..., None] * (rank[..., None] == slots).astype(jnp.float32)
    select = jnp.transpose(select, (0, 2, 3, 1))
    slot_gate = jnp.einsum('bect,bte->bec', select, gate_sum)
    return select, slot_gate


def reference(cotangent, routes, gates, gate_pre, up_pre, w_gate, w_up, w_down):
    blocks = N_DP * N_EXPERT
    split = N_EXPERT // EXP_FL
    hidden = FFE // split
    state = cotangent
    total = jnp.zeros((N_PIPE, EXP_FL * FFE, D), jnp.float32)
    for step in range(STEPS):
        produced = []
        for section in range(N_PIPE):
            grad_in = state[section].reshape(blocks, TOK_DEV, D)
            ids = routes[section, step].reshape(blocks, TOK_DEV, TOPK)
            weights = gates[section, step].reshape(blocks, TOK_DEV, TOPK)
            select, slot_gate = slot_tables(ids, weights)
            rows = jnp.einsum('bect,btd->becd', select, grad_in.astype(jnp.float32)).astype(jnp.bfloat16)
            grad_out = grad_in.astype(jnp.float32)
            pre_gate_all = gate_pre[section, step].reshape(blocks * CAP, EXP_FL * FFE)
            pre_up_all = up_pre[section, step].reshape(blocks * CAP, EXP_FL * FFE)
            for expert in range(EXP_FL):
                lower = expert * FFE
                flat_rows = rows[:, expert].reshape(blocks * CAP, D)
                gate_col = slot_gate[:, expert].reshape(blocks * CAP, 1)
                pre_u = pre_gate_all[:, lower:lower + FFE].astype(jnp.float32)
                pre_v = pre_up_all[:, lower:lower + FFE].astype(jnp.float32)
                down_rows = w_down[section, lower:lower + FFE]
                grad_act = gate_col * jnp.dot(flat_rows, down_rows.T, preferred_element_type=jnp.float32)
                sig = jax.nn.sigmoid(pre_u)
                act = pre_u * sig
                dsilu = sig * (1.0 + pre_u * (1.0 - sig))
                d_gate = (grad_act * pre_v * dsilu).astype(jnp.bfloat16)
                d_up = (grad_act * act).astype(jnp.bfloat16)
                scaled = (gate_col * act * pre_v).astype(jnp.bfloat16)
                term = jnp.dot(scaled.T, flat_rows, preferred_element_type=jnp.float32)
                total = total.at[section, lower:lower + FFE].add(term)
                if step + 1 < STEPS:
                    gate_cols = w_gate[section][:, lower:lower + FFE].reshape(D, split, hidden).astype(jnp.float32)
                    up_cols = w_up[section][:, lower:lower + FFE].reshape(D, split, hidden).astype(jnp.float32)
                    dg = d_gate.reshape(blocks * CAP, split, hidden).astype(jnp.float32)
                    du = d_up.reshape(blocks * CAP, split, hidden).astype(jnp.float32)
                    parts = jnp.einsum('rjh,djh->jrd', dg, gate_cols) + jnp.einsum('rjh,djh->jrd', du, up_cols)
                    parts = parts.astype(jnp.bfloat16).astype(jnp.float32)
                    summed = jnp.sum(parts, axis=0).reshape(blocks, CAP, D)
                    grad_out = grad_out + jnp.einsum('bct,bcd->btd', select[:, expert], summed)
            produced.append(grad_out.astype(jnp.bfloat16).reshape(TOKENS, D))
        if step + 1 < STEPS:
            state = jnp.stack(produced[1:] + [jnp.zeros((TOKENS, D), jnp.bfloat16)])
    return total
```

```python
import functools

import jax
import jax.numpy as jnp
from jax import lax
from jax.experimental import pallas as pl
from jax.experimental.pallas import tpu as pltpu
from jax.sharding import PartitionSpec as P

EXP_FL = 2
STEPS = 2
LANES = 128
MESH = pl.DeviceIdType.MESH
F32 = jnp.float32
BF16 = jnp.bfloat16


def contract_last(left, right):
    return lax.dot_general(
        left, right, (((1,), (1,)), ((), ())), preferred_element_type=F32
    )


def steps_of(size):
    for count in range(2, size // 32 + 1, 2):
        if size % count == 0 and size // count % 16 == 0 and size // count <= 448:
            return size // count
    return 0


def rows_dot(x, weight, start, size, columns):
    m = x.shape[0]
    held = (size // 2 - m // 2) // 16 * 16
    right = jnp.concatenate([weight[start : start + held, columns], x], axis=0)
    left = jnp.concatenate([x, weight[start + held : start + size, columns]], axis=0)
    return contract_last(left, right)


def rows_out(both, m):
    held = both.shape[1] - m
    low = held // LANES * LANES
    streamed = both[m:, low : held + m].T[held - low :, :]
    return jnp.concatenate([both[0:m, 0:held], streamed], axis=1)


def slot_table(ids, weights, capacity):
    topk, tokens = ids.shape
    row = lax.broadcasted_iota(jnp.int32, (8, tokens), 0)
    expert = row // capacity
    hit = jnp.zeros((8, tokens), F32)
    gate = jnp.zeros((8, tokens), F32)
    for k in range(topk):
        match = ids[k : k + 1, :] == expert
        hit = jnp.where(match, 1.0, hit)
        gate = gate + jnp.where(match, weights[k : k + 1, :], 0.0)
    upto = (
        lax.broadcasted_iota(jnp.int32, (tokens, tokens), 0)
        <= lax.broadcasted_iota(jnp.int32, (tokens, tokens), 1)
    ).astype(F32)
    rank = jnp.dot(hit.astype(BF16), upto.astype(BF16), preferred_element_type=F32) - 1.0
    valid = (rank == (row % capacity).astype(F32)) & (row < EXP_FL * capacity)
    select = jnp.where(valid, hit, 0.0)
    slot_gate = jnp.sum(select * gate, axis=1, keepdims=True)
    return select, jnp.broadcast_to(slot_gate, (8, LANES))


def kernel(
    dims,
    cot_hbm,
    routes_hbm,
    gates_hbm,
    pre_u,
    pre_v,
    w_gate,
    w_up,
    w_down,
    out_rows,
    out_scaled,
    cot,
    routes,
    gates,
    wd,
    wg,
    wu,
    got_u,
    got_v,
    stage_u,
    stage_v,
    send_rows,
    recv_rows,
    stage_x,
    sel_send,
    sel_recv,
    base_send,
    base_recv,
    acc_send,
    acc_recv,
    part_send,
    part_recv,
    fin_stage,
    fin_send,
    fin_recv,
    cot_sem,
    w_sem,
    pre_ss,
    pre_rs,
    rows_ss,
    rows_rs,
    sel_ss,
    sel_rs,
    base_ss,
    base_rs,
    acc_ss,
    acc_rs,
    part_ss,
    part_rs,
    fin_ss,
    fin_rs,
):
    n_pipe, n_dp, n_exp, cap, width, hidden, n_ch = dims
    half = width // n_dp
    ch = half // n_ch
    split = n_exp // EXP_FL
    n_src = n_dp * n_exp
    slots = n_src * cap
    group = n_dp * cap
    n_h, part_h = acc_send.shape[0], acc_send.shape[2]
    step_h, step_c = steps_of(part_h), steps_of(ch)
    fast = slots == 16 and step_h > 64 and step_c > 64 and part_h % LANES == 0
    p, r, j = lax.axis_index("pipe"), lax.axis_index("dp"), lax.axis_index("expert")
    me = j * n_dp + r

    def at(pipe, dp, expert):
        return {"pipe": pipe, "dp": dp, "expert": expert}

    def remote(src, dst, ss, rs, where):
        return pltpu.make_async_remote_copy(
            src_ref=src, dst_ref=dst, send_sem=ss, recv_sem=rs, device_id=where, device_id_type=MESH
        )

    def weight_copies():
        downs, outs = [], []
        for k in range(n_ch):
            at_col = pl.multiple_of(r * half + k * ch, LANES)
            downs.append(
                pltpu.make_async_copy(w_down.at[0, :, pl.ds(at_col, ch)], wd.at[k], w_sem.at[0, k])
            )
        for k in range(n_ch):
            at_col = pl.multiple_of(r * half + k * ch, LANES)
            outs.append(
                (
                    pltpu.make_async_copy(w_gate.at[0, pl.ds(at_col, ch), :], wg.at[k], w_sem.at[1, k]),
                    pltpu.make_async_copy(w_up.at[0, pl.ds(at_col, ch), :], wu.at[k], w_sem.at[2, k]),
                )
            )
        return downs, outs

    cot_copy = pltpu.make_async_copy(cot_hbm.at[0], cot, cot_sem.at[0])
    routes_copy = pltpu.make_async_copy(routes_hbm.at[0], routes, cot_sem.at[1])
    gates_copy = pltpu.make_async_copy(gates_hbm.at[0], gates, cot_sem.at[2])
    routes_copy.start()
    gates_copy.start()
    cot_copy.start()

    local_u = pltpu.make_async_copy(pre_u.at[0, :, 0], got_u.at[r], pre_rs.at[0, 0])
    local_v = pltpu.make_async_copy(pre_v.at[0, :, 0], got_v.at[r], pre_rs.at[1, 0])
    local_u.start()
    local_v.start()

    barrier = pltpu.get_barrier_semaphore()
    for o in range(1, n_src):
        q = lax.rem(me + o, n_src)
        pl.semaphore_signal(
            barrier, inc=1, device_id=at(p, lax.rem(q, n_dp), q // n_dp), device_id_type=MESH
        )

    @pl.when(p > 0)
    def _():
        for s in range(n_exp):
            pl.semaphore_signal(barrier, inc=1, device_id=at(p - 1, r, s), device_id_type=MESH)

    @pl.when(p < n_pipe - 1)
    def _():
        for s in range(n_exp):
            pl.semaphore_signal(barrier, inc=1, device_id=at(p + 1, r, s), device_id_type=MESH)

    routes_copy.wait()
    gates_copy.wait()
    local_u.wait()
    local_v.wait()

    @pl.when(p > 0)
    def _():
        downs, outs = weight_copies()
        for copy in downs:
            copy.start()
        for a, b in outs:
            a.start()
            b.start()

    sel0, g0 = slot_table(routes[0], gates[0].astype(F32), cap)
    sel1, g1 = slot_table(routes[1], gates[1].astype(F32), cap)
    sel_send[:, 0 : sel1.shape[1]] = sel1
    cot_copy.wait()

    for d in range(n_dp):
        rows = jnp.dot(
            sel0.astype(BF16), cot[:, d * half : (d + 1) * half], preferred_element_type=F32
        )
        for e in range(EXP_FL):
            send_rows[d, e, :, 0:half] = rows[e * cap : (e + 1) * cap].astype(BF16)
            send_rows[d, e, :, half : half + LANES] = g0[e * cap : (e + 1) * cap].astype(BF16)
            send_rows[d, e, :, half + LANES : half + 2 * LANES] = g1[e * cap : (e + 1) * cap].astype(BF16)
    recv_rows[me] = send_rows[r, j // split]

    above = (p + n_pipe - 1) // n_pipe
    below = (2 * n_pipe - 2 - p) // n_pipe
    pl.semaphore_wait(barrier, n_src - 1 + n_exp * (above + below))

    def rows_copy(o):
        q = lax.rem(me + o, n_src)
        dp_q, exp_q = lax.rem(q, n_dp), q // n_dp
        return remote(
            send_rows.at[dp_q, exp_q // split], recv_rows.at[me], rows_ss.at[o], rows_rs.at[me], at(p, dp_q, exp_q)
        )

    def rows_got(o):
        q = lax.rem(me + o, n_src)
        return remote(
            send_rows.at[0, 0], recv_rows.at[q], rows_ss.at[o], rows_rs.at[q], at(p, lax.rem(q, n_dp), q // n_dp)
        )

    for o in range(1, n_src):
        rows_copy(o).start()

    def sel_copy():
        return remote(sel_send, sel_recv, sel_ss.at[0], sel_rs.at[0], at(p + 1, r, j))

    @pl.when(p < n_pipe - 1)
    def _():
        sel_copy().start()

    def pre_copies(o):
        d = lax.rem(r + o, n_dp)
        return (
            remote(got_u.at[r], got_u.at[r], pre_ss.at[0, o], pre_rs.at[0, o], at(p, d, j)),
            remote(got_v.at[r], got_v.at[r], pre_ss.at[1, o], pre_rs.at[1, o], at(p, d, j)),
        )

    for o in range(1, n_dp):
        for copy in pre_copies(o):
            copy.start()

    def base_copy(o):
        d = lax.rem(r + o, n_dp)
        return remote(base_send.at[d], base_recv.at[r], base_ss.at[o], base_rs.at[o], at(p, d, j))

    @pl.when(p > 0)
    def _():
        sel_p = remote(sel_send, sel_recv, sel_ss.at[0], sel_rs.at[0], at(p - 1, r, j))
        sel_p.wait_recv()
        nxt = sel_recv[:, 0 : sel0.shape[1]]
        mapping = contract_last(nxt, sel0)
        pad = jnp.zeros((8, LANES - mapping.shape[1]), F32)
        mapping = jnp.concatenate([mapping, pad], axis=1)
        for d in range(n_dp):
            base_send[d, :, 0:half] = jnp.dot(
                nxt.astype(BF16), cot[:, d * half : (d + 1) * half], preferred_element_type=F32
            )
            base_send[d, :, half : half + LANES] = mapping
        base_recv[r] = base_send[r]
        for o in range(1, n_dp):
            base_copy(o).start()

    def acc_copy(h, o):
        d = lax.rem(r + o, n_dp)
        return remote(
            acc_send.at[h], acc_recv.at[h, o], acc_ss.at[h, o], acc_rs.at[h, o], at(p, d, j)
        )

    for o in range(1, n_src):
        rows_got(o).wait_recv()
    for q in range(n_src):
        stage_x[q * cap : (q + 1) * cap, :] = recv_rows[q].astype(F32)
    x = stage_x[:, 0:half].astype(BF16)
    out_rows[0:slots, :] = x

    @pl.when(p > 0)
    def _():
        downs, _ = weight_copies()
        for k in range(n_ch):
            downs[k].wait()
        for h in range(n_h):
            if fast:
                pieces = []
                for i in range(h * part_h, (h + 1) * part_h, step_h):
                    both = None
                    for k in range(n_ch):
                        term = rows_dot(
                            stage_x[:, k * ch : (k + 1) * ch].astype(BF16), wd.at[k], i, step_h, slice(0, ch)
                        )
                        both = term if both is None else both + term
                    pieces.append(rows_out(both, slots))
                acc_send[h] = jnp.concatenate(pieces, axis=1)
            else:
                acc = jnp.zeros((slots, part_h), F32)
                for k in range(n_ch):
                    acc = acc + contract_last(
                        stage_x[:, k * ch : (k + 1) * ch].astype(BF16), wd[k, h * part_h : (h + 1) * part_h, :]
                    )
                acc_send[h] = acc
            for o in range(1, n_dp):
                acc_copy(h, o).start()

    for o in range(1, n_dp):
        for copy in pre_copies(o):
            copy.wait_recv()
    for t in range(STEPS):
        for s in range(n_exp):
            for d in range(n_dp):
                row = t * slots + (s * n_dp + d) * cap
                stage_u[row : row + cap, :] = got_u[d, t, s].astype(F32)
                stage_v[row : row + cap, :] = got_v[d, t, s].astype(F32)
    for t in range(STEPS):
        u = stage_u[t * slots : (t + 1) * slots, :]
        v = stage_v[t * slots : (t + 1) * slots, :]
        g = stage_x[:, half + t * LANES : half + t * LANES + 1]
        out_scaled[t * slots : (t + 1) * slots, :] = (g * (u * jax.nn.sigmoid(u)) * v).astype(BF16)

    def part_copy(k, o):
        s = lax.rem(j + o, n_exp)
        return remote(
            part_send.at[k, s], part_recv.at[k, j], part_ss.at[k, o], part_rs.at[k, o], at(p, r, s)
        )

    def part_got(k, o):
        s = lax.rem(j + n_exp - o, n_exp)
        return remote(
            part_send.at[k, s], part_recv.at[k, s], part_ss.at[k, o], part_rs.at[k, o], at(p, r, s)
        )

    def fin_copy(k, s):
        return remote(
            fin_send.at[k, s // split], fin_recv.at[k, j], fin_ss.at[k, s], fin_rs.at[k, j], at(p - 1, r, s)
        )

    @pl.when(p > 0)
    def _():
        _, outs = weight_copies()

        def pre_grads(h):
            at_h = slice(h * part_h, (h + 1) * part_h)
            u = stage_u[0:slots, at_h]
            v = stage_v[0:slots, at_h]
            g = stage_x[:, half : half + 1]
            sig = jax.nn.sigmoid(u)
            total = acc_send[h]
            for o in range(1, n_dp):
                acc_copy(h, o).wait_recv()
                total = total + acc_recv[h, o]
            d_act = g * total
            d_gate = (d_act * v * (sig * (1.0 + u * (1.0 - sig)))).astype(BF16)
            d_up = (d_act * (u * sig)).astype(BF16)
            return d_gate, d_up

        def shares_of(k, d_gate, d_up):
            if not fast:
                yield contract_last(d_gate, wg[k]) + contract_last(d_up, wu[k])
                return
            everything = slice(0, hidden)
            for i in range(0, ch, step_c):
                yield rows_out(
                    rows_dot(d_gate, wg.at[k], i, step_c, everything)
                    + rows_dot(d_up, wu.at[k], i, step_c, everything),
                    slots,
                )

        def send_parts(k, pieces):
            part = jnp.concatenate(pieces, axis=1)
            for s in range(n_exp):
                part_send[k, s] = part[s * group : (s + 1) * group].astype(BF16)
            part_recv[k, j] = part_send[k, j]
            for o in range(1, n_exp):
                part_copy(k, o).start()

        for k in range(n_ch):
            outs[k][0].wait()
            outs[k][1].wait()
        d_gate, d_up = pre_grads(n_h - 1)
        ready = None
        for k in range(n_ch):
            pieces = []
            for i, piece in enumerate(shares_of(k, d_gate, d_up)):
                pieces.append(piece)
                if ready is not None and i == 1:
                    send_parts(*ready)
                    ready = None
            if ready is not None:
                send_parts(*ready)
            ready = (k, pieces)
        send_parts(*ready)
        for o in range(1, n_dp):
            base_copy(o).wait_recv()

        def reduce(k):
            for o in range(1, n_exp):
                part_got(k, o).wait_recv()
            sums = []
            for e in range(EXP_FL):
                value = part_recv[k, e * split].astype(F32)
                for i in range(1, split):
                    value = value + part_recv[k, e * split + i].astype(F32)
                sums.append(value)
            for d in range(n_dp):
                new = base_recv[d, :, k * ch : (k + 1) * ch]
                for e in range(EXP_FL):
                    for c in range(cap):
                        at_slot = half + e * cap + c
                        row = d * cap + c
                        new = new + base_recv[d, :, at_slot : at_slot + 1] * sums[e][row : row + 1]
                for e in range(EXP_FL):
                    fin_stage[e, d * cap : (d + 1) * cap, :] = new[e * cap : (e + 1) * cap]
            for e in range(EXP_FL):
                fin_send[k, e] = fin_stage[e].astype(BF16)
            for s in range(n_exp):
                fin_copy(k, s).start()

        for k in range(n_ch):
            reduce(k)

    @pl.when(p < n_pipe - 1)
    def _():
        for k in range(n_ch):
            for s in range(n_exp):
                remote(
                    fin_send.at[k, 0], fin_recv.at[k, s], fin_ss.at[k, s], fin_rs.at[k, s], at(p + 1, r, s)
                ).wait_recv()
            for s in range(n_exp):
                stage_x[s * group : (s + 1) * group, k * ch : (k + 1) * ch] = fin_recv[k, s].astype(F32)
        out_rows[slots : 2 * slots, :] = stage_x[:, 0:half].astype(BF16)

    @pl.when(p == n_pipe - 1)
    def _():
        out_rows[slots : 2 * slots, :] = jnp.zeros((slots, half), BF16)

    for o in range(1, n_src):
        rows_copy(o).wait_send()
    for o in range(1, n_dp):
        for copy in pre_copies(o):
            copy.wait_send()

    @pl.when(p < n_pipe - 1)
    def _():
        sel_copy().wait_send()

    @pl.when(p > 0)
    def _():
        for o in range(1, n_dp):
            base_copy(o).wait_send()
            for h in range(n_h):
                acc_copy(h, o).wait_send()
        for k in range(n_ch):
            for o in range(1, n_exp):
                part_copy(k, o).wait_send()
            for s in range(n_exp):
                fin_copy(k, s).wait_send()


def output_blocks(rows):
    sizes = [16, 16, 32, 64]
    sizes += [LANES] * (rows // LANES - 1)
    return [(sum(sizes[:i]), size) for i, size in enumerate(sizes)]


def output_kernel(rows, scaled, out, held, sem):
    right = rows[...]
    copies = []
    for i, (first, size) in enumerate(output_blocks(out.shape[1])):
        at = pl.ds(first, size)
        held[at, :] = lax.dot_general(
            scaled[:, at], right, (((0,), (0,)), ((), ())), preferred_element_type=F32
        )
        copies.append(pltpu.make_async_copy(held.at[at, :], out.at[0, at, :], sem.at[i]))
        copies[-1].start()
    for copy in copies:
        copy.wait()


def body(mesh_shape, cotangent, routes, gates, gate_pre, up_pre, w_gate, w_up, w_down):
    n_pipe, n_dp, n_exp = mesh_shape
    width = cotangent.shape[2]
    cap = gate_pre.shape[4]
    hidden = gate_pre.shape[5]
    half = width // n_dp
    n_ch = 2
    ch = half // n_ch
    n_h = 1
    n_src = n_dp * n_exp
    slots = n_src * cap
    group = n_dp * cap
    dims = (n_pipe, n_dp, n_exp, cap, width, hidden, n_ch)
    vmem = pl.BlockSpec(memory_space=pltpu.VMEM)
    hbm = pl.BlockSpec(memory_space=pltpu.HBM)
    dma = pltpu.SemaphoreType.DMA
    rows, scaled = pl.pallas_call(
        functools.partial(kernel, dims),
        out_shape=(
            pltpu.VMEM((STEPS * slots, half), BF16),
            pltpu.VMEM((STEPS * slots, hidden), BF16),
        ),
        in_specs=[hbm, hbm, hbm, hbm, hbm, hbm, hbm, hbm],
        out_specs=(vmem, vmem),
        scratch_shapes=[
            pltpu.VMEM((cotangent.shape[1], width), BF16),
            pltpu.VMEM((STEPS, routes.shape[3], routes.shape[2]), jnp.int32),
            pltpu.VMEM((STEPS, routes.shape[3], routes.shape[2]), BF16),
            pltpu.VMEM((n_ch, hidden, ch), BF16),
            pltpu.VMEM((n_ch, ch, hidden), BF16),
            pltpu.VMEM((n_ch, ch, hidden), BF16),
            pltpu.VMEM((n_dp, STEPS, n_exp, cap, hidden), BF16),
            pltpu.VMEM((n_dp, STEPS, n_exp, cap, hidden), BF16),
            pltpu.VMEM((STEPS * slots, hidden), F32),
            pltpu.VMEM((STEPS * slots, hidden), F32),
            pltpu.VMEM((n_dp, EXP_FL, cap, half + 2 * LANES), BF16),
            pltpu.VMEM((n_src, cap, half + 2 * LANES), BF16),
            pltpu.VMEM((slots, half + 2 * LANES), F32),
            pltpu.VMEM((8, LANES), F32),
            pltpu.VMEM((8, LANES), F32),
            pltpu.VMEM((n_dp, 8, half + LANES), F32),
            pltpu.VMEM((n_dp, 8, half + LANES), F32),
            pltpu.VMEM((n_h, slots, hidden // n_h), F32),
            pltpu.VMEM((n_h, n_dp, slots, hidden // n_h), F32),
            pltpu.VMEM((n_ch, n_exp, group, ch), BF16),
            pltpu.VMEM((n_ch, n_exp, group, ch), BF16),
            pltpu.VMEM((EXP_FL, group, ch), F32),
            pltpu.VMEM((n_ch, EXP_FL, group, ch), BF16),
            pltpu.VMEM((n_ch, n_exp, group, ch), BF16),
            dma((3,)),
            dma((3, n_ch)),
            dma((2, n_dp)),
            dma((2, n_dp)),
            dma((n_src,)),
            dma((n_src,)),
            dma((1,)),
            dma((1,)),
            dma((n_dp,)),
            dma((n_dp,)),
            dma((n_h, n_dp)),
            dma((n_h, n_dp)),
            dma((n_ch, n_exp)),
            dma((n_ch, n_exp)),
            dma((n_ch, n_exp)),
            dma((n_ch, n_exp)),
        ],
        compiler_params=pltpu.CompilerParams(
            collective_id=0, has_side_effects=True, vmem_limit_bytes=58 * 1024 * 1024
        ),
    )(cotangent, jnp.swapaxes(routes, 2, 3), jnp.swapaxes(gates, 2, 3), gate_pre, up_pre, w_gate, w_up, w_down)
    total = pl.pallas_call(
        output_kernel,
        out_shape=jax.ShapeDtypeStruct((1, hidden, half), F32),
        in_specs=[vmem, vmem],
        out_specs=hbm,
        scratch_shapes=[pltpu.VMEM((hidden, half), F32), dma((len(output_blocks(hidden)),))],
        compiler_params=pltpu.CompilerParams(vmem_limit_bytes=60 * 1024 * 1024),
    )(pltpu.with_memory_space_constraint(rows, pltpu.VMEM), pltpu.with_memory_space_constraint(scaled, pltpu.VMEM))
    return total


def solution(mesh):
    mesh_shape = (mesh.shape["pipe"], mesh.shape["dp"], mesh.shape["expert"])
    in_specs = (
        P("pipe", ("dp", "expert"), None),
        P("pipe", None, ("dp", "expert"), None),
        P("pipe", None, ("dp", "expert"), None),
        P("pipe", None, "dp", None, None, "expert"),
        P("pipe", None, "dp", None, None, "expert"),
        P("pipe", None, "expert"),
        P("pipe", None, "expert"),
        P("pipe", "expert", None),
    )
    out_specs = P("pipe", "expert", "dp")
    return jax.shard_map(
        functools.partial(body, mesh_shape), mesh=mesh, in_specs=in_specs, out_specs=out_specs, check_vma=False
    )
```

```python
import functools

import jax
import jax.numpy as jnp
from jax import lax
from jax.experimental import pallas as pl
from jax.experimental.pallas import tpu as pltpu
from jax.sharding import PartitionSpec as P

EXP_FL = 2
STEPS = 2
LANES = 128
STEP = 512
MESH = pl.DeviceIdType.MESH
F32 = jnp.float32
BF16 = jnp.bfloat16


def contract_last(left, right):
    return lax.dot_general(
        left, right, (((1,), (1,)), ((), ())), preferred_element_type=F32
    )


def steps_of(size):
    for count in range(2, size // 32 + 1, 2):
        if size % count == 0 and size // count % 16 == 0 and size // count <= STEP:
            return size // count
    return 0


def rows_dot(x, weight, start, size, columns):
    m = x.shape[0]
    held = (size // 2 - m // 2) // 16 * 16
    right = jnp.concatenate([weight[start : start + held, columns], x], axis=0)
    left = jnp.concatenate([x, weight[start + held : start + size, columns]], axis=0)
    return contract_last(left, right)


def rows_out(both, m):
    held = both.shape[1] - m
    low = held // LANES * LANES
    streamed = both[m:, low : held + m].T[held - low :, :]
    return jnp.concatenate([both[0:m, 0:held], streamed], axis=1)


def slot_table(ids, weights, capacity):
    topk, tokens = ids.shape
    row = lax.broadcasted_iota(jnp.int32, (8, tokens), 0)
    expert = row // capacity
    hit = jnp.zeros((8, tokens), F32)
    gate = jnp.zeros((8, tokens), F32)
    for k in range(topk):
        match = ids[k : k + 1, :] == expert
        hit = jnp.where(match, 1.0, hit)
        gate = gate + jnp.where(match, weights[k : k + 1, :], 0.0)
    upto = (
        lax.broadcasted_iota(jnp.int32, (tokens, tokens), 0)
        <= lax.broadcasted_iota(jnp.int32, (tokens, tokens), 1)
    ).astype(F32)
    rank = jnp.dot(hit.astype(BF16), upto.astype(BF16), preferred_element_type=F32) - 1.0
    valid = (rank == (row % capacity).astype(F32)) & (row < EXP_FL * capacity)
    select = jnp.where(valid, hit, 0.0)
    slot_gate = jnp.sum(select * gate, axis=1, keepdims=True)
    return select, jnp.broadcast_to(slot_gate, (8, LANES))


def kernel(
    dims,
    cot_hbm,
    routes_hbm,
    gates_hbm,
    pre_u,
    pre_v,
    w_gate,
    w_up,
    w_down,
    out_rows,
    out_scaled,
    cot,
    routes,
    gates,
    wd,
    wg,
    wu,
    got_u,
    got_v,
    stage_u,
    stage_v,
    send_rows,
    recv_rows,
    stage_x,
    sel_send,
    sel_recv,
    base_send,
    base_recv,
    acc_send,
    acc_recv,
    part_send,
    part_recv,
    fin_stage,
    fin_send,
    fin_recv,
    cot_sem,
    w_sem,
    pre_ss,
    pre_rs,
    rows_ss,
    rows_rs,
    sel_ss,
    sel_rs,
    base_ss,
    base_rs,
    acc_ss,
    acc_rs,
    part_ss,
    part_rs,
    fin_ss,
    fin_rs,
):
    n_pipe, n_dp, n_exp, cap, width, hidden, n_ch = dims
    half = width // n_dp
    ch = half // n_ch
    split = n_exp // EXP_FL
    n_src = n_dp * n_exp
    slots = n_src * cap
    group = n_dp * cap
    n_h, part_h = acc_send.shape[0], acc_send.shape[2]
    step_h, step_c = steps_of(part_h), steps_of(ch)
    fast = slots == 16 and step_h > 64 and step_c > 64 and part_h % LANES == 0
    p, r, j = lax.axis_index("pipe"), lax.axis_index("dp"), lax.axis_index("expert")
    me = j * n_dp + r
    far = lax.rem(2 * n_exp - 1 - 2 * j, n_exp)
    offsets = [lax.rem(far + i, n_exp) for i in range(0, n_exp, 2)] + list(range(2, n_exp, 2))
    peers = [(o, d) for o in offsets for d in range(n_dp)] + [(0, d) for d in range(1, n_dp)]

    def at(pipe, dp, expert):
        return {"pipe": pipe, "dp": dp, "expert": expert}

    def remote(src, dst, ss, rs, where):
        return pltpu.make_async_remote_copy(
            src_ref=src, dst_ref=dst, send_sem=ss, recv_sem=rs, device_id=where, device_id_type=MESH
        )

    def weight_copies():
        downs, outs = [], []
        for k in range(n_ch):
            at_col = pl.multiple_of(r * half + k * ch, LANES)
            downs.append(
                pltpu.make_async_copy(w_down.at[0, :, pl.ds(at_col, ch)], wd.at[k], w_sem.at[0, k])
            )
        for k in range(n_ch):
            at_col = pl.multiple_of(r * half + k * ch, LANES)
            outs.append(
                (
                    pltpu.make_async_copy(w_gate.at[0, pl.ds(at_col, ch), :], wg.at[k], w_sem.at[1, k]),
                    pltpu.make_async_copy(w_up.at[0, pl.ds(at_col, ch), :], wu.at[k], w_sem.at[2, k]),
                )
            )
        return downs, outs

    cot_copy = pltpu.make_async_copy(cot_hbm.at[0], cot, cot_sem.at[0])
    routes_copy = pltpu.make_async_copy(routes_hbm.at[0], routes, cot_sem.at[1])
    gates_copy = pltpu.make_async_copy(gates_hbm.at[0], gates, cot_sem.at[2])
    routes_copy.start()
    gates_copy.start()
    cot_copy.start()

    local_u = pltpu.make_async_copy(pre_u.at[0, :, 0], got_u.at[r], pre_rs.at[0, 0])
    local_v = pltpu.make_async_copy(pre_v.at[0, :, 0], got_v.at[r], pre_rs.at[1, 0])
    local_u.start()
    local_v.start()

    @pl.when(p > 0)
    def _():
        downs, outs = weight_copies()
        for copy in downs:
            copy.start(priority=1)
        for a, b in outs:
            a.start(priority=1)
            b.start(priority=1)

    barrier = pltpu.get_barrier_semaphore()
    for o in range(1, n_src):
        q = lax.rem(me + o, n_src)
        pl.semaphore_signal(
            barrier, inc=1, device_id=at(p, lax.rem(q, n_dp), q // n_dp), device_id_type=MESH
        )

    @pl.when(p > 0)
    def _():
        pl.semaphore_signal(barrier, inc=1, device_id=at(p - 1, r, j), device_id_type=MESH)

    @pl.when(p < n_pipe - 1)
    def _():
        pl.semaphore_signal(barrier, inc=1, device_id=at(p + 1, r, j), device_id_type=MESH)

    routes_copy.wait()
    gates_copy.wait()
    sel0, g0 = slot_table(routes[0], gates[0].astype(F32), cap)
    sel1, g1 = slot_table(routes[1], gates[1].astype(F32), cap)
    sel_send[:, 0 : sel1.shape[1]] = sel1
    cot_copy.wait()

    for d in range(n_dp):
        rows = jnp.dot(
            sel0.astype(BF16), cot[:, d * half : (d + 1) * half], preferred_element_type=F32
        )
        for e in range(EXP_FL):
            send_rows[d, e, :, 0:half] = rows[e * cap : (e + 1) * cap].astype(BF16)
            send_rows[d, e, :, half : half + LANES] = g0[e * cap : (e + 1) * cap].astype(BF16)
            send_rows[d, e, :, half + LANES : half + 2 * LANES] = g1[e * cap : (e + 1) * cap].astype(BF16)
    recv_rows[me] = send_rows[r, j // split]

    above = (p + n_pipe - 1) // n_pipe
    below = (2 * n_pipe - 2 - p) // n_pipe
    pl.semaphore_wait(barrier, n_src - 1 + above + below)

    def peer(i):
        o, d = peers[i]
        return lax.rem(r + d, n_dp), lax.rem(j + o, n_exp)

    def rows_copy(i):
        dp_q, exp_q = peer(i)
        return remote(
            send_rows.at[dp_q, exp_q // split], recv_rows.at[me], rows_ss.at[i], rows_rs.at[me], at(p, dp_q, exp_q)
        )

    def rows_got(i):
        dp_q, exp_q = peer(i)
        q = exp_q * n_dp + dp_q
        return remote(send_rows.at[0, 0], recv_rows.at[q], rows_ss.at[i], rows_rs.at[q], at(p, dp_q, exp_q))

    for i in range(n_src - 1):
        rows_copy(i).start()

    def sel_copy():
        return remote(sel_send, sel_recv, sel_ss.at[0], sel_rs.at[0], at(p + 1, r, j))

    @pl.when(p < n_pipe - 1)
    def _():
        sel_copy().start()

    def pre_copies(o):
        d = lax.rem(r + o, n_dp)
        return (
            remote(got_u.at[r], got_u.at[r], pre_ss.at[0, o], pre_rs.at[0, o], at(p, d, j)),
            remote(got_v.at[r], got_v.at[r], pre_ss.at[1, o], pre_rs.at[1, o], at(p, d, j)),
        )

    local_u.wait()
    local_v.wait()
    for o in range(1, n_dp):
        for copy in pre_copies(o):
            copy.start()

    def base_copy(o):
        d = lax.rem(r + o, n_dp)
        return remote(base_send.at[d], base_recv.at[r], base_ss.at[o], base_rs.at[o], at(p, d, j))

    @pl.when(p > 0)
    def _():
        sel_p = remote(sel_send, sel_recv, sel_ss.at[0], sel_rs.at[0], at(p - 1, r, j))
        sel_p.wait_recv()
        nxt = sel_recv[:, 0 : sel0.shape[1]]
        mapping = contract_last(nxt, sel0)
        pad = jnp.zeros((8, LANES - mapping.shape[1]), F32)
        mapping = jnp.concatenate([mapping, pad], axis=1)
        for d in range(n_dp):
            base_send[d, :, 0:half] = jnp.dot(
                nxt.astype(BF16), cot[:, d * half : (d + 1) * half], preferred_element_type=F32
            )
            base_send[d, :, half : half + LANES] = mapping
        base_recv[r] = base_send[r]
        for o in range(1, n_dp):
            base_copy(o).start()

    def acc_copy(h, o):
        d = lax.rem(r + o, n_dp)
        return remote(
            acc_send.at[h], acc_recv.at[h, o], acc_ss.at[h, o], acc_rs.at[h, o], at(p, d, j)
        )

    for i in range(n_src - 1):
        rows_got(i).wait_recv()
    for q in range(n_src):
        stage_x[q * cap : (q + 1) * cap, :] = recv_rows[q].astype(F32)
    x = stage_x[:, 0:half].astype(BF16)
    out_rows[0:slots, :] = x

    @pl.when(p > 0)
    def _():
        downs, _ = weight_copies()
        for k in range(n_ch):
            downs[k].wait()
        for h in range(n_h):
            if fast:
                pieces = []
                for i in range(h * part_h, (h + 1) * part_h, step_h):
                    both = None
                    for k in range(n_ch):
                        term = rows_dot(
                            stage_x[:, k * ch : (k + 1) * ch].astype(BF16), wd.at[k], i, step_h, slice(0, ch)
                        )
                        both = term if both is None else both + term
                    pieces.append(rows_out(both, slots))
                acc_send[h] = jnp.concatenate(pieces, axis=1)
            else:
                acc = jnp.zeros((slots, part_h), F32)
                for k in range(n_ch):
                    acc = acc + contract_last(
                        stage_x[:, k * ch : (k + 1) * ch].astype(BF16), wd[k, h * part_h : (h + 1) * part_h, :]
                    )
                acc_send[h] = acc
            for o in range(1, n_dp):
                acc_copy(h, o).start()

    for o in range(1, n_dp):
        for copy in pre_copies(o):
            copy.wait_recv()
    for t in range(STEPS):
        for s in range(n_exp):
            for d in range(n_dp):
                row = t * slots + (s * n_dp + d) * cap
                stage_u[row : row + cap, :] = got_u[d, t, s].astype(F32)
                stage_v[row : row + cap, :] = got_v[d, t, s].astype(F32)
    for t in range(STEPS):
        u = stage_u[t * slots : (t + 1) * slots, :]
        v = stage_v[t * slots : (t + 1) * slots, :]
        g = stage_x[:, half + t * LANES : half + t * LANES + 1]
        out_scaled[t * slots : (t + 1) * slots, :] = (g * (u * jax.nn.sigmoid(u)) * v).astype(BF16)

    def part_copy(k, o):
        s = lax.rem(j + o, n_exp)
        return remote(
            part_send.at[k, s], part_recv.at[k, j], part_ss.at[k, o], part_rs.at[k, o], at(p, r, s)
        )

    def part_got(k, o):
        s = lax.rem(j + n_exp - o, n_exp)
        return remote(
            part_send.at[k, s], part_recv.at[k, s], part_ss.at[k, o], part_rs.at[k, o], at(p, r, s)
        )

    def fin_copy(k, s):
        return remote(
            fin_send.at[k, s // split], fin_recv.at[k, j], fin_ss.at[k, s], fin_rs.at[k, j], at(p - 1, r, s)
        )

    @pl.when(p > 0)
    def _():
        _, outs = weight_copies()

        def pre_grads(h):
            at_h = slice(h * part_h, (h + 1) * part_h)
            u = stage_u[0:slots, at_h]
            v = stage_v[0:slots, at_h]
            g = stage_x[:, half : half + 1]
            sig = jax.nn.sigmoid(u)
            total = acc_send[h]
            for o in range(1, n_dp):
                acc_copy(h, o).wait_recv()
                total = total + acc_recv[h, o]
            d_act = g * total
            d_gate = (d_act * v * (sig * (1.0 + u * (1.0 - sig)))).astype(BF16)
            d_up = (d_act * (u * sig)).astype(BF16)
            return d_gate, d_up

        def shares_of(k, d_gate, d_up):
            if not fast:
                yield contract_last(d_gate, wg[k]) + contract_last(d_up, wu[k])
                return
            everything = slice(0, hidden)
            for i in range(0, ch, step_c):
                yield rows_out(
                    rows_dot(d_gate, wg.at[k], i, step_c, everything)
                    + rows_dot(d_up, wu.at[k], i, step_c, everything),
                    slots,
                )

        def send_parts(k, pieces):
            part = jnp.concatenate(pieces, axis=1)
            for s in range(n_exp):
                part_send[k, s] = part[s * group : (s + 1) * group].astype(BF16)
            part_recv[k, j] = part_send[k, j]
            for o in offsets:
                part_copy(k, o).start()

        for k in range(n_ch):
            outs[k][0].wait()
            outs[k][1].wait()
        d_gate, d_up = pre_grads(n_h - 1)
        ready = None
        for k in range(n_ch):
            pieces = []
            for i, piece in enumerate(shares_of(k, d_gate, d_up)):
                pieces.append(piece)
                if ready is not None and i == 1:
                    send_parts(*ready)
                    ready = None
            if ready is not None:
                send_parts(*ready)
            ready = (k, pieces)
        send_parts(*ready)
        for o in range(1, n_dp):
            base_copy(o).wait_recv()

        def reduce(k):
            for o in range(1, n_exp):
                part_got(k, o).wait_recv()
            sums = []
            for e in range(EXP_FL):
                value = part_recv[k, e * split].astype(F32)
                for i in range(1, split):
                    value = value + part_recv[k, e * split + i].astype(F32)
                sums.append(value)
            for d in range(n_dp):
                new = base_recv[d, :, k * ch : (k + 1) * ch]
                for e in range(EXP_FL):
                    for c in range(cap):
                        at_slot = half + e * cap + c
                        row = d * cap + c
                        new = new + base_recv[d, :, at_slot : at_slot + 1] * sums[e][row : row + 1]
                for e in range(EXP_FL):
                    fin_stage[e, d * cap : (d + 1) * cap, :] = new[e * cap : (e + 1) * cap]
            for e in range(EXP_FL):
                fin_send[k, e] = fin_stage[e].astype(BF16)
            for o in offsets + [0]:
                fin_copy(k, lax.rem(j + o, n_exp)).start()

        for k in range(n_ch):
            reduce(k)

    @pl.when(p < n_pipe - 1)
    def _():
        for k in range(n_ch):
            for s in range(n_exp):
                remote(
                    fin_send.at[k, 0], fin_recv.at[k, s], fin_ss.at[k, s], fin_rs.at[k, s], at(p + 1, r, s)
                ).wait_recv()
            for s in range(n_exp):
                stage_x[s * group : (s + 1) * group, k * ch : (k + 1) * ch] = fin_recv[k, s].astype(F32)
        out_rows[slots : 2 * slots, :] = stage_x[:, 0:half].astype(BF16)

    @pl.when(p == n_pipe - 1)
    def _():
        out_rows[slots : 2 * slots, :] = jnp.zeros((slots, half), BF16)

    for i in range(n_src - 1):
        rows_copy(i).wait_send()
    for o in range(1, n_dp):
        for copy in pre_copies(o):
            copy.wait_send()

    @pl.when(p < n_pipe - 1)
    def _():
        sel_copy().wait_send()

    @pl.when(p > 0)
    def _():
        for o in range(1, n_dp):
            base_copy(o).wait_send()
            for h in range(n_h):
                acc_copy(h, o).wait_send()
        for k in range(n_ch):
            for o in range(1, n_exp):
                part_copy(k, o).wait_send()
            for s in range(n_exp):
                fin_copy(k, s).wait_send()


def output_blocks(rows):
    sizes = [16, 16, 32, 64]
    sizes += [LANES] * (rows // LANES - 1)
    return [(sum(sizes[:i]), size) for i, size in enumerate(sizes)]


def output_kernel(rows, scaled, out, held, sem):
    right = rows[...]
    copies = []
    for i, (first, size) in enumerate(output_blocks(out.shape[1])):
        at = pl.ds(first, size)
        held[at, :] = lax.dot_general(
            scaled[:, at], right, (((0,), (0,)), ((), ())), preferred_element_type=F32
        )
        copies.append(pltpu.make_async_copy(held.at[at, :], out.at[0, at, :], sem.at[i]))
        copies[-1].start()
    for copy in copies:
        copy.wait()


def body(mesh_shape, cotangent, routes, gates, gate_pre, up_pre, w_gate, w_up, w_down):
    n_pipe, n_dp, n_exp = mesh_shape
    width = cotangent.shape[2]
    cap = gate_pre.shape[4]
    hidden = gate_pre.shape[5]
    half = width // n_dp
    n_ch = 2
    ch = half // n_ch
    n_h = 1
    n_src = n_dp * n_exp
    slots = n_src * cap
    group = n_dp * cap
    dims = (n_pipe, n_dp, n_exp, cap, width, hidden, n_ch)
    vmem = pl.BlockSpec(memory_space=pltpu.VMEM)
    hbm = pl.BlockSpec(memory_space=pltpu.HBM)
    dma = pltpu.SemaphoreType.DMA
    rows, scaled = pl.pallas_call(
        functools.partial(kernel, dims),
        out_shape=(
            pltpu.VMEM((STEPS * slots, half), BF16),
            pltpu.VMEM((STEPS * slots, hidden), BF16),
        ),
        in_specs=[hbm, hbm, hbm, hbm, hbm, hbm, hbm, hbm],
        out_specs=(vmem, vmem),
        scratch_shapes=[
            pltpu.VMEM((cotangent.shape[1], width), BF16),
            pltpu.VMEM((STEPS, routes.shape[3], routes.shape[2]), jnp.int32),
            pltpu.VMEM((STEPS, routes.shape[3], routes.shape[2]), BF16),
            pltpu.VMEM((n_ch, hidden, ch), BF16),
            pltpu.VMEM((n_ch, ch, hidden), BF16),
            pltpu.VMEM((n_ch, ch, hidden), BF16),
            pltpu.VMEM((n_dp, STEPS, n_exp, cap, hidden), BF16),
            pltpu.VMEM((n_dp, STEPS, n_exp, cap, hidden), BF16),
            pltpu.VMEM((STEPS * slots, hidden), F32),
            pltpu.VMEM((STEPS * slots, hidden), F32),
            pltpu.VMEM((n_dp, EXP_FL, cap, half + 2 * LANES), BF16),
            pltpu.VMEM((n_src, cap, half + 2 * LANES), BF16),
            pltpu.VMEM((slots, half + 2 * LANES), F32),
            pltpu.VMEM((8, LANES), F32),
            pltpu.VMEM((8, LANES), F32),
            pltpu.VMEM((n_dp, 8, half + LANES), F32),
            pltpu.VMEM((n_dp, 8, half + LANES), F32),
            pltpu.VMEM((n_h, slots, hidden // n_h), F32),
            pltpu.VMEM((n_h, n_dp, slots, hidden // n_h), F32),
            pltpu.VMEM((n_ch, n_exp, group, ch), BF16),
            pltpu.VMEM((n_ch, n_exp, group, ch), BF16),
            pltpu.VMEM((EXP_FL, group, ch), F32),
            pltpu.VMEM((n_ch, EXP_FL, group, ch), BF16),
            pltpu.VMEM((n_ch, n_exp, group, ch), BF16),
            dma((3,)),
            dma((3, n_ch)),
            dma((2, n_dp)),
            dma((2, n_dp)),
            dma((n_src,)),
            dma((n_src,)),
            dma((1,)),
            dma((1,)),
            dma((n_dp,)),
            dma((n_dp,)),
            dma((n_h, n_dp)),
            dma((n_h, n_dp)),
            dma((n_ch, n_exp)),
            dma((n_ch, n_exp)),
            dma((n_ch, n_exp)),
            dma((n_ch, n_exp)),
        ],
        compiler_params=pltpu.CompilerParams(
            collective_id=0, has_side_effects=True, vmem_limit_bytes=58 * 1024 * 1024
        ),
    )(cotangent, jnp.swapaxes(routes, 2, 3), jnp.swapaxes(gates, 2, 3), gate_pre, up_pre, w_gate, w_up, w_down)
    total = pl.pallas_call(
        output_kernel,
        out_shape=jax.ShapeDtypeStruct((1, hidden, half), F32),
        in_specs=[vmem, vmem],
        out_specs=hbm,
        scratch_shapes=[pltpu.VMEM((hidden, half), F32), dma((len(output_blocks(hidden)),))],
        compiler_params=pltpu.CompilerParams(vmem_limit_bytes=60 * 1024 * 1024),
    )(pltpu.with_memory_space_constraint(rows, pltpu.VMEM), pltpu.with_memory_space_constraint(scaled, pltpu.VMEM))
    return total


def solution(mesh):
    mesh_shape = (mesh.shape["pipe"], mesh.shape["dp"], mesh.shape["expert"])
    in_specs = (
        P("pipe", ("dp", "expert"), None),
        P("pipe", None, ("dp", "expert"), None),
        P("pipe", None, ("dp", "expert"), None),
        P("pipe", None, "dp", None, None, "expert"),
        P("pipe", None, "dp", None, None, "expert"),
        P("pipe", None, "expert"),
        P("pipe", None, "expert"),
        P("pipe", "expert", None),
    )
    out_specs = P("pipe", "expert", "dp")
    return jax.shard_map(
        functools.partial(body, mesh_shape), mesh=mesh, in_specs=in_specs, out_specs=out_specs, check_vma=False
    )
```
